32 devices in a mesh: groups: 2 (over x), gx: 8 (over z, y), gy: 2 (over core).
Axes of the slice: x: 2, y: 2, z: 4, core: 2. Of those that a mesh axis runs over, the one named last changes fastest.
Arguments:
- tokens: bfloat16 [2, 1024, 7168], P(None, ('groups', 'gx', 'gy')), parts along dimension 1, may hold values from -6 to 6
- expert_ids: int32 [2, 1024, 2], P(None, ('groups', 'gx', 'gy')), parts along dimension 1, may hold values from 0 to 3, all different within a row; in each aligned block of 32 rows (0 to 31, 32 to 63, ..., all dimensions but the last counted through in order) at most 20 rows name the same one
- gate_weights: float32 [2, 1024, 2], P(None, ('groups', 'gx', 'gy')), parts along dimension 1, may hold values from 0.1 to 1
- w_gate: bfloat16 [8, 7168, 512], P('gx', None, 'gy'), may hold values from -0.0625 to 0.0625
- w_up: bfloat16 [8, 7168, 512], P('gx', None, 'gy'), may hold values from -0.0625 to 0.0625
- w_down: bfloat16 [8, 512, 7168], P('gx', 'gy'), may hold values from -0.1875 to 0.1875
Outputs:
- combined: bfloat16 [2, 1024, 7168], P(None, ('groups', 'gx', 'gy')), parts along dimension 1
The draws below stay inside these ranges and needn't reach their ends.
There are 2 independent parts, one for each index of `groups`. The reference program is written for one: setup_inputs(seed, part) draws one part's arguments, and reference() takes and returns one part's arrays. A program takes and returns all parts, laid end to end along the dimension named above; an argument that names none is the same for every part. Nothing has to cross between parts.
Inputs may be any that keep to these rules, and one draw needn't show every extreme that they name: `expert_ids`: each row names 2 different experts. Within the 32 rows of one device and one micro-batch no expert is named more than 20 times, and in some such blocks one is named exactly 20 times.
All inputs are finite; a program needn't handle non-finite values.
Results may differ from the reference program's by a relative error of at most 0.012.
Values may be sent and summed in bfloat16 or wider, within the bound.
No kernel may reach another device: no remote copies, remote signals or barrier semaphores. Data moves between devices by JAX's collectives and lax.ppermute only.
A program may use at most 192 MiB of HBM per device.

```python
import math
import jax
import jax.numpy as jnp
import numpy as np
from jax import lax

D = 7168
FFW = 1024
TOPK = 2
MB = 2
ROWS = 32
EXPERTS = 4
CAP = 20
TOKENS = 512
N_GX = 8
N_GY = 2


def steps_of(rng, dims, shards, low, top_value):
    gain, own = 1.0, jax.random.fold_in(rng, 6)
    for axis_at, blocks in shards:
        steps = jnp.exp(jax.random.uniform(jax.random.fold_in(own, axis_at), (blocks,), jnp.float32, low / len(shards), top_value / len(shards)))
        gain = gain * jnp.repeat(steps, dims[axis_at] // blocks).reshape([-1 if axis == axis_at else 1 for axis in range(len(dims))])
    return gain


def shared_out(stream_key, own, number, rows, count, top, most, lean):
    ranking = jax.random.permutation(stream_key, count)
    packed, ordinary = shares(count, rows * top, most, lean, True), shares(count, rows * top, most, lean, False)
    places = jnp.arange(count)

    def named(sizes, rotation):
        used = int((sizes > 0).sum())
        fixed = max(1, used // 4)
        passed = fixed + (places - fixed + rotation * (used - fixed)) % max(1, count - fixed)
        return jnp.zeros((count,), jnp.int32).at[ranking[jnp.where(places < fixed, places, passed)]].set(jnp.asarray(sizes, jnp.int32))

    sizes = jnp.where(number % 4 == 0, named(packed, number // 4), named(ordinary, number - number // 4 - 1))
    mixed = jax.random.permutation(jax.random.fold_in(own, 3), count)
    source_of, sink = mixed[0:count // 2 * 2:2], mixed[1:count // 2 * 2:2]
    margin = jnp.minimum(sizes[source_of] - 1, most - sizes[sink]) // 2
    margin = jnp.where((source_of == ranking[0]) | (sink == ranking[0]) | (sizes[sink] == 0), 0, jnp.maximum(margin, 0))
    passed = jax.random.randint(jax.random.fold_in(own, 4), (count // 2,), 0, 1 << 20) % (margin + 1)
    sizes = sizes.at[source_of].add(-passed).at[sink].add(passed)
    labels = jnp.searchsorted(jnp.cumsum(sizes), jnp.arange(rows * top), side="right").astype(jnp.int32)
    table = labels.reshape(top, rows).T
    table = table[jax.random.permutation(jax.random.fold_in(own, 1), rows)]
    rotation = jax.random.randint(jax.random.fold_in(own, 2), (rows, 1), 0, top)
    return jnp.take_along_axis(table, (jnp.arange(top)[None, :] + rotation) % top, axis=1)


def shares(amount, total, most, lean, full):
    portions = [(1 << 20) // math.isqrt(standing ** lean) + 1 for standing in range(1, amount + 1)]
    largest = most if full else min(most, max(-(-total // amount), total * portions[0] // sum(portions)))
    least = 1 if total - largest >= amount - 1 else 0
    given, surplus = [largest] + [least] * (amount - 1), total - largest - least * (amount - 1)
    while surplus > 0:
        candidates = [i for i in range(1, amount) if given[i] < largest] or [i for i in range(1, amount) if given[i] < most]
        pool, remaining = sum([portions[i] for i in candidates]), surplus
        for i in candidates:
            addition = min(most - given[i], max(1, remaining * portions[i] // pool), surplus)
            given[i] = given[i] + addition
            surplus = surplus - addition
    return np.array(given)


def scatter_about(stream_key, extent, deviation, most, split=(), kind=jnp.bfloat16):
    factor_of = steps_of(stream_key, extent, split, -0.22, 0.18) if split else 1.0
    drawn = jax.random.normal(stream_key, extent, jnp.float32) * deviation * factor_of
    return jnp.minimum(jnp.maximum(drawn, -most), most).astype(kind)


def setup_inputs(seed: int = 0, part: int = 0) -> dict:
    keys = jax.random.split(jax.random.key(seed), 7)
    part_splits = jax.random.split(jax.random.fold_in(keys[6], part), 7)
    tokens = scatter_about(part_splits[0], (MB, TOKENS, D), 1.0, 6.0, ((1, 16),))
    expert_ids_keys = jax.random.split(jax.random.fold_in(part_splits[1], 1), MB * TOKENS // ROWS)
    expert_ids_turns = jax.random.permutation(jax.random.fold_in(part_splits[1], 3), MB * TOKENS // ROWS)
    expert_ids = jax.vmap(lambda own, number: shared_out(jax.random.fold_in(part_splits[1], 2), own, number, ROWS, EXPERTS, TOPK, CAP, 1))(expert_ids_keys, expert_ids_turns).reshape((MB, TOKENS, TOPK))
    gate_weights = jnp.clip(jnp.exp(math.log(1.0) - 2.3025851 * jax.random.uniform(part_splits[2], (MB, TOKENS, TOPK), jnp.float32) ** steps_of(part_splits[2], (MB, TOKENS, TOPK), ((1, 16),), -0.2, 0.2)), 0.1, 1.0)
    w_gate = scatter_about(keys[3], (2 * EXPERTS, D, FFW // 2), D ** -0.5, 0.0625, ((0, 8), (2, 2)))
    w_up = scatter_about(keys[4], (2 * EXPERTS, D, FFW // 2), D ** -0.5, 0.0625, ((0, 8), (2, 2)))
    w_down = scatter_about(keys[5], (2 * EXPERTS, FFW // 2, D), FFW ** -0.5, 0.1875, ((0, 8), (1, 2)))
    return dict(tokens=tokens, expert_ids=expert_ids, gate_weights=gate_weights, w_gate=w_gate, w_up=w_up, w_down=w_down)


def reference(tokens, expert_ids, gate_weights, w_gate, w_up, w_down):
    devices = N_GX * N_GY
    quarter = FFW // (2 * N_GY)
    ids = expert_ids.reshape(MB, devices, ROWS * TOPK)
    marks = (ids[..., None] == jnp.arange(EXPERTS, dtype=jnp.int32)).astype(jnp.int32)
    before = jnp.cumsum(marks, axis=2) - marks
    slot = jnp.sum(before * marks, axis=-1).reshape(MB, devices, ROWS, TOPK)
    chosen = ids.reshape(MB, devices, ROWS, TOPK)
    token_rows = tokens.reshape(MB, devices, ROWS, D).astype(jnp.float32)
    gates = gate_weights.reshape(MB, devices, ROWS, TOPK).astype(jnp.float32)
    slot_iota = jnp.arange(CAP, dtype=jnp.int32)

    def one_expert(total, inputs):
        index, wg, wu, wd = inputs
        hit = ((chosen == index)[..., None] & (slot[..., None] == slot_iota)).astype(jnp.float32)
        pick = jnp.sum(hit, axis=3)
        mixing = jnp.sum(hit * gates[..., None], axis=3)
        buffer = jnp.einsum("mdrc,mdrf->mdcf", pick, token_rows).astype(jnp.bfloat16).reshape(-1, D)
        halves = []
        for half_index in range(2):
            summed = jnp.zeros((buffer.shape[0], D), jnp.float32)
            for slice_index in range(N_GY):
                low = slice_index * quarter
                gate = jnp.dot(buffer, wg[half_index][:, low:low + quarter], preferred_element_type=jnp.float32)
                up = jnp.dot(buffer, wu[half_index][:, low:low + quarter], preferred_element_type=jnp.float32)
                hidden = (jax.nn.silu(gate) * up).astype(jnp.bfloat16)
                partial_value = jnp.dot(hidden, wd[half_index][low:low + quarter, :], preferred_element_type=jnp.float32)
                summed = summed + partial_value.astype(jnp.bfloat16).astype(jnp.float32)
            halves.append(summed.astype(jnp.bfloat16).astype(jnp.float32))
        expert_out = (halves[0] + halves[1]).reshape(MB, devices, CAP, D)
        total = total + jnp.einsum("mdrc,mdcf->mdrf", mixing, expert_out, precision=lax.Precision.HIGHEST)
        return total, None

    start = jnp.zeros((MB, devices, ROWS, D), jnp.float32)
    inputs = (jnp.arange(EXPERTS, dtype=jnp.int32),
              w_gate.reshape(EXPERTS, 2, D, FFW // 2),
              w_up.reshape(EXPERTS, 2, D, FFW // 2),
              w_down.reshape(EXPERTS, 2, FFW // 2, D))
    total, unused = lax.scan(one_expert, start, inputs)
    return total.astype(jnp.bfloat16).reshape(MB, devices * ROWS, D)
```

```python
import jax
import jax.numpy as jnp
from jax import lax
from jax.sharding import PartitionSpec as P

FORWARD_CHUNKS = 2
RETURN_CHUNKS = 4


def swapped(value, mask):
    return lax.ppermute(value, "gx", [(i, i ^ mask) for i in range(lax.axis_size("gx"))])


def columns(width, count):
    while width % (count * 128):
        count -= 1
    step = width // count
    return [(i * step, (i + 1) * step) for i in range(count)]


def slot_places(chosen, home, capacity):
    batches, rows, topk = chosen.shape
    flat = chosen.reshape(batches, rows * topk)
    earlier = jnp.arange(rows * topk)[None, :] < jnp.arange(rows * topk)[:, None]
    same = (flat[:, :, None] == flat[:, None, :]) & earlier[None]
    slot = jnp.sum(same.astype(jnp.int32), axis=2)
    batch = jnp.arange(batches, dtype=jnp.int32)[:, None]
    place = ((flat ^ home) * batches + batch) * capacity + slot
    return place.reshape(batches * rows, topk)


def body(tokens, expert_ids, gate_weights, w_gate, w_up, w_down):
    batches, rows, width = tokens.shape
    topk = expert_ids.shape[2]
    experts = lax.axis_size("gx") // 2
    capacity = 2 * min(rows // 2, (5 * rows * topk + 8 * experts - 1) // (8 * experts))
    group = batches * capacity
    full_gate = lax.all_gather(w_gate[0], "gy", axis=1, tiled=True)
    full_up = lax.all_gather(w_up[0], "gy", axis=1, tiled=True)
    full_down = lax.all_gather(w_down[0], "gy", axis=0, tiled=True)

    place = slot_places(expert_ids, lax.axis_index("gx") // 2, capacity)
    gates = gate_weights.reshape(batches * rows, topk)
    token_rows = tokens.reshape(batches * rows, width)
    order = list(range(1, experts))[::-1]

    pickers, mixings = [], []
    for r in range(experts):
        targets = r * group + jnp.arange(group, dtype=jnp.int32)
        hit = (place.T[:, None, :] == targets[None, :, None]).astype(jnp.float32)
        pickers.append(jnp.sum(hit, axis=0).astype(jnp.bfloat16))
        hit = (place[:, :, None] == targets[None, None, :]).astype(jnp.float32)
        mixings.append(jnp.sum(hit * gates[:, :, None], axis=1))

    gate = up = None
    for low, high in columns(width, FORWARD_CHUNKS):
        own = [None] * experts
        for r in order + [0]:
            piece = jnp.dot(
                pickers[r], token_rows[:, low:high], preferred_element_type=jnp.float32
            ).astype(jnp.bfloat16)
            own[r] = swapped(piece, 2 * r) if r else piece
        partner = [swapped(piece, 1) for piece in own]
        slot_rows = jnp.concatenate(own + partner, axis=0)
        g = jnp.dot(slot_rows, full_gate[low:high], preferred_element_type=jnp.float32)
        u = jnp.dot(slot_rows, full_up[low:high], preferred_element_type=jnp.float32)
        gate = g if gate is None else gate + g
        up = u if up is None else up + u
    hidden = (jax.nn.silu(gate) * up).astype(jnp.bfloat16)
    half = experts * group

    results = []
    for low, high in columns(width, RETURN_CHUNKS):
        down = full_down[:, low:high]
        theirs = jnp.dot(hidden[half:], down, preferred_element_type=jnp.float32)
        arrived = swapped(theirs.astype(jnp.bfloat16), 1)
        mine = jnp.dot(hidden[:half], down, preferred_element_type=jnp.float32)
        summed = (mine + arrived.astype(jnp.float32)).astype(jnp.bfloat16)
        mixed = None
        for r in [0] + order:
            piece = summed[r * group : (r + 1) * group]
            if r:
                piece = swapped(piece, 2 * r)
            term = jnp.dot(
                mixings[r],
                piece.astype(jnp.float32),
                precision=lax.Precision.HIGHEST,
                preferred_element_type=jnp.float32,
            )
            mixed = term if mixed is None else mixed + term
        results.append(mixed.astype(jnp.bfloat16))
    return jnp.concatenate(results, axis=1).reshape(batches, rows, width)


def solution(mesh):
    placed = (
        P(None, ("groups", "gx", "gy"), None),
        P(None, ("groups", "gx", "gy"), None),
        P(None, ("groups", "gx", "gy"), None),
        P("gx", None, "gy"),
        P("gx", None, "gy"),
        P("gx", "gy", None),
    )
    return jax.shard_map(
        body,
        mesh=mesh,
        in_specs=placed,
        out_specs=P(None, ("groups", "gx", "gy"), None),
        check_vma=False,
    )
```

```python
import jax
import jax.numpy as jnp
from jax import lax
from jax.sharding import PartitionSpec as P

FORWARD_CHUNKS = 2
RETURN_CHUNKS = 4


def swapped(value, axis, mask):
    return lax.ppermute(value, axis, [(i, i ^ mask) for i in range(lax.axis_size(axis))])


def columns(width, count):
    while width % (count * 128):
        count -= 1
    step = width // count
    return [(i * step, (i + 1) * step) for i in range(count)]


def slot_places(chosen, home, capacity):
    batches, rows, topk = chosen.shape
    flat = chosen.reshape(batches, rows * topk)
    earlier = jnp.arange(rows * topk)[None, :] < jnp.arange(rows * topk)[:, None]
    same = (flat[:, :, None] == flat[:, None, :]) & earlier[None]
    slot = jnp.sum(same.astype(jnp.int32), axis=2)
    batch = jnp.arange(batches, dtype=jnp.int32)[:, None]
    place = ((flat ^ home) * batches + batch) * capacity + slot
    return place.reshape(batches * rows, topk)


def body(tokens, expert_ids, gate_weights, w_gate, w_up, w_down):
    batches, rows, width = tokens.shape
    topk = expert_ids.shape[2]
    experts = lax.axis_size("gx") // 2
    capacity = 2 * min(rows // 2, (5 * rows * topk + 8 * experts - 1) // (8 * experts))
    group = batches * capacity
    shares = [(w_gate[0], w_up[0], w_down[0])]
    shares.append(tuple(swapped(weight, "gy", 1) for weight in shares[0]))

    place = slot_places(expert_ids, lax.axis_index("gx") // 2, capacity)
    gates = gate_weights.reshape(batches * rows, topk)
    token_rows = tokens.reshape(batches * rows, width)
    order = list(range(1, experts))[::-1]

    pickers, mixings = [], []
    for r in range(experts):
        targets = r * group + jnp.arange(group, dtype=jnp.int32)
        hit = (place.T[:, None, :] == targets[None, :, None]).astype(jnp.float32)
        pickers.append(jnp.sum(hit, axis=0).astype(jnp.bfloat16))
        hit = (place[:, :, None] == targets[None, None, :]).astype(jnp.float32)
        mixings.append(jnp.sum(hit * gates[:, :, None], axis=1))

    sums = None
    for low, high in columns(width, FORWARD_CHUNKS):
        own = [None] * experts
        for r in order + [0]:
            piece = jnp.dot(
                pickers[r], token_rows[:, low:high], preferred_element_type=jnp.float32
            ).astype(jnp.bfloat16)
            own[r] = swapped(piece, "gx", 2 * r) if r else piece
        partner = [swapped(piece, "gx", 1) for piece in own]
        if sums is not None:
            partner[1], sums = lax.optimization_barrier((partner[1], sums))
        slot_rows = jnp.concatenate(own + partner, axis=0)
        terms = [
            jnp.dot(slot_rows, weight[low:high], preferred_element_type=jnp.float32)
            for share in shares
            for weight in share[:2]
        ]
        sums = terms if sums is None else [s + t for s, t in zip(sums, terms)]
    hidden = [
        (jax.nn.silu(gate) * up).astype(jnp.bfloat16) for gate, up in zip(sums[::2], sums[1::2])
    ]
    half = experts * group

    results = []
    for low, high in columns(width, RETURN_CHUNKS):
        def down(begin, end):
            return sum(
                jnp.dot(
                    rows_of[begin:end], share[2][:, low:high], preferred_element_type=jnp.float32
                )
                for rows_of, share in zip(hidden, shares)
            )

        arrived = swapped(down(half, 2 * half).astype(jnp.bfloat16), "gx", 1)
        summed = (down(0, half) + arrived.astype(jnp.float32)).astype(jnp.bfloat16)
        mixed = None
        for r in [0] + order:
            piece = summed[r * group : (r + 1) * group]
            if r:
                piece = swapped(piece, "gx", 2 * r)
            term = jnp.dot(
                mixings[r],
                piece.astype(jnp.float32),
                precision=lax.Precision.HIGHEST,
                preferred_element_type=jnp.float32,
            )
            mixed = term if mixed is None else mixed + term
        results.append(mixed.astype(jnp.bfloat16))
    return jnp.concatenate(results, axis=1).reshape(batches, rows, width)


def solution(mesh):
    placed = (
        P(None, ("groups", "gx", "gy"), None),
        P(None, ("groups", "gx", "gy"), None),
        P(None, ("groups", "gx", "gy"), None),
        P("gx", None, "gy"),
        P("gx", None, "gy"),
        P("gx", "gy", None),
    )
    return jax.shard_map(
        body,
        mesh=mesh,
        in_specs=placed,
        out_specs=P(None, ("groups", "gx", "gy"), None),
        check_vma=False,
    )
```
